32 devices in a mesh: dp: 16 (over z, x, core), tensor: 2 (over y).
Axes of the slice: x: 2, y: 2, z: 4, core: 2. Of those that a mesh axis runs over, the one named last changes fastest.
Arguments:
- inputs: bfloat16 [16384, 768], P(('dp', 'tensor')), may hold values from -6 to 6
- lengths: int32 [16], P('dp'), may hold values from 512 to 1024, as said below
- query_weight: bfloat16 [768, 768], P(None, 'tensor'), may hold values from -0.21875 to 0.21875
- query_bias: float32 [768], P('tensor'), may hold values from -3 to 3
- key_weight: bfloat16 [768, 768], P(None, 'tensor'), may hold values from -0.21875 to 0.21875
- value_weight: bfloat16 [768, 768], P(None, 'tensor'), may hold values from -0.21875 to 0.21875
- value_bias: float32 [768], P('tensor'), may hold values from -3 to 3
- proj_weight: bfloat16 [768, 768], P('tensor'), may hold values from -4 to 4
- proj_bias: float32 [768], replicated, may hold values from -3 to 3
- attn_gain: float32 [768], replicated, may hold values from 0.1 to 1.9
- attn_shift: float32 [768], replicated, may hold values from -2 to 2
- up_weight: bfloat16 [768, 3072], P(None, 'tensor'), may hold values from -0.21875 to 0.21875
- up_bias: float32 [3072], P('tensor'), may hold values from -3 to 3
- down_weight: bfloat16 [3072, 768], P('tensor'), may hold values from -0.109375 to 0.109375
- down_bias: float32 [768], replicated, may hold values from -3 to 3
- ffn_gain: float32 [768], replicated, may hold values from 0.1 to 1.9
- ffn_shift: float32 [768], replicated, may hold values from -2 to 2
- filter_couple_scores: float32 [12, 512, 512], P('tensor', 'dp'), may hold values from -5 to 5
- filter_smoothing_jitter: float32 [12, 512, 512], P('tensor', 'dp'), may hold values from -5 to 5
- cotangent: bfloat16 [16384, 768], P(('dp', 'tensor')), may hold values from -6 to 6
Outputs:
- layer_output: bfloat16 [16384, 768], P(('dp', 'tensor'))
- input_grads: bfloat16 [16384, 768], P(('dp', 'tensor'))
- query_grads: float32 [768, 768], P(None, 'tensor')
- key_grads: float32 [768, 768], P(None, 'tensor')
- value_grads: float32 [768, 768], P(None, 'tensor')
- proj_grads: float32 [768, 768], P('tensor')
- up_grads: float32 [768, 3072], P(None, 'tensor')
- down_grads: float32 [3072, 768], P('tensor')
- query_bias_grads: float32 [768], P('tensor')
- value_bias_grads: float32 [768], P('tensor')
- up_bias_grads: float32 [3072], P('tensor')
- proj_bias_grads: float32 [768], replicated
- down_bias_grads: float32 [768], replicated
- attn_gain_grads: float32 [768], replicated
- attn_shift_grads: float32 [768], replicated
- ffn_gain_grads: float32 [768], replicated
- ffn_shift_grads: float32 [768], replicated
- mask_logit_gradients: float32 [12, 512, 512], P('tensor', 'dp')
The draws below stay inside these ranges and needn't reach their ends.
Inputs may be any that keep to these rules, and one draw needn't show every extreme that they name: Each sequence's live slots are its first lengths[b]; at least one sequence fills all 1024 slots.
All inputs are finite; a program needn't handle non-finite values.
Results may differ from the reference program's by a relative error of at most 0.015.
Values may be sent and summed in bfloat16 or wider, within the bound.
A program may use at most 192 MiB of HBM per device.

```python
import math
import jax
import jax.numpy as jnp
from jax import lax

D = 768
HEADS = 12
HEAD_DIM = 64
FF = 3072
WIN = 512
SEQ = 1024
SEQS = 16
TOKENS = 16384


def draw_lengths(key, part):
    sampled = jax.random.randint(key, (SEQS,), SEQ // 2, SEQ + 1, dtype=jnp.int32)
    full_slot = jax.random.randint(jax.random.fold_in(key, 7), (), 0, SEQS, dtype=jnp.int32)
    positions = jnp.arange(SEQS, dtype=jnp.int32)
    return jnp.where(positions == full_slot, SEQ, sampled).astype(jnp.int32)


def level_of(rng, extent, shards, least, top_value):
    def one(dim, blocks):
        steps = jax.random.uniform(jax.random.fold_in(jax.random.fold_in(rng, 6), dim), (blocks,), jnp.float32, least / len(shards), top_value / len(shards))
        return jnp.repeat(jnp.exp(steps), extent[dim] // blocks).reshape((-1,) + (1,) * (len(extent) - dim - 1))

    factor_of = one(*shards[0])
    for cut in shards[1:]:
        factor_of = factor_of * one(*cut)
    return factor_of


def centred(rng, shape, scale, reach, split=(), kind=jnp.bfloat16):
    entries = scale * jax.random.normal(rng, shape, jnp.float32)
    if split:
        entries = entries * level_of(rng, shape, split, -0.22, 0.18)
    return jnp.clip(entries, -reach, reach).astype(kind)


def setup_inputs(seed: int = 0) -> dict:
    seeds = jax.random.split(jax.random.key(seed), 21)
    inputs = centred(seeds[0], (TOKENS, D), 1.0, 6.0, ((0, 32),))
    lengths = draw_lengths(jax.random.fold_in(seeds[20], 71), 0)
    query_weight = centred(seeds[2], (D, D), D ** -0.5, 0.21875, ((1, 2),))
    query_bias = centred(seeds[3], (D,), 0.5, 3.0, ((0, 2),), jnp.float32)
    key_weight = centred(seeds[4], (D, D), D ** -0.5, 0.21875, ((1, 2),))
    value_weight = centred(seeds[5], (D, D), D ** -0.5, 0.21875, ((1, 2),))
    value_bias = centred(seeds[6], (D,), 0.5, 3.0, ((0, 2),), jnp.float32)
    proj_weight = centred(seeds[7], (D, D), 2 ** -0.5, 4.0, ((0, 2),))
    proj_bias = centred(seeds[8], (D,), 0.5, 3.0, (), jnp.float32)
    attn_gain = jnp.clip(1.0 + 0.18 * jax.random.normal(seeds[9], (D,), jnp.float32), 0.1, 1.9)
    attn_shift = centred(seeds[10], (D,), 0.3, 2.0, (), jnp.float32)
    up_weight = centred(seeds[11], (D, FF), D ** -0.5, 0.21875, ((1, 2),))
    up_bias = centred(seeds[12], (FF,), 0.5, 3.0, ((0, 2),), jnp.float32)
    down_weight = centred(seeds[13], (FF, D), FF ** -0.5, 0.109375, ((0, 2),))
    down_bias = centred(seeds[14], (D,), 0.5, 3.0, (), jnp.float32)
    ffn_gain = jnp.clip(1.0 + 0.18 * jax.random.normal(seeds[15], (D,), jnp.float32), 0.1, 1.9)
    ffn_shift = centred(seeds[16], (D,), 0.3, 2.0, (), jnp.float32)
    filter_couple_scores = centred(seeds[17], (HEADS, WIN, WIN), 1.0, 5.0, ((0, 2), (1, 16)), jnp.float32)
    filter_smoothing_jitter = centred(seeds[18], (HEADS, WIN, WIN), 1.0, 5.0, ((0, 2), (1, 16)), jnp.float32)
    cotangent = centred(seeds[19], (TOKENS, D), 1.0, 6.0, ((0, 32),))
    return {"inputs": inputs, "lengths": lengths, "query_weight": query_weight, "query_bias": query_bias, "key_weight": key_weight, "value_weight": value_weight, "value_bias": value_bias, "proj_weight": proj_weight, "proj_bias": proj_bias, "attn_gain": attn_gain, "attn_shift": attn_shift, "up_weight": up_weight, "up_bias": up_bias, "down_weight": down_weight, "down_bias": down_bias, "ffn_gain": ffn_gain, "ffn_shift": ffn_shift, "filter_couple_scores": filter_couple_scores, "filter_smoothing_jitter": filter_smoothing_jitter, "cotangent": cotangent}


@jax.custom_vjp
def reduced_accuracy(v):
    return lax.optimization_barrier(v.astype(jnp.bfloat16)).astype(jnp.float32)

@jax.custom_vjp
def low_back(v):
    return v

def low_keep(v):
    return (reduced_accuracy(v), None)

def low_pass(kept, grad):
    return (grad,)

def back_keep(v):
    return (v, None)

def back_low(kept, grad):
    return (reduced_accuracy(grad),)
reduced_accuracy.defvjp(low_keep, low_pass)
low_back.defvjp(back_keep, back_low)
softening_heat = 0.5
epsilon = 1e-05

def matmul(left_side, right_side):
    return jnp.dot(left_side, right_side, precision=lax.Precision.HIGHEST)

def layer_norm(values, gain, shift):
    centre = values - lax.optimization_barrier(jnp.mean(values, axis=-1, keepdims=True))
    spread = lax.optimization_barrier(jnp.mean(centre * centre, axis=-1, keepdims=True))
    return centre * lax.rsqrt(spread + epsilon) * gain + shift

def forward(params, seq_rows, live_slots, draw_jitter):
    query_weight, query_bias, key_weight, value_weight, value_bias, proj_weight, proj_bias, attn_gain, attn_shift, up_weight, up_bias, down_weight, down_bias, ffn_gain, ffn_shift, filter_couple_scores = params
    trainable_focus_filter = reduced_accuracy(jax.nn.sigmoid((filter_couple_scores + draw_jitter) / softening_heat))
    queries = reduced_accuracy(low_back(matmul(seq_rows, query_weight) + query_bias)).reshape(SEQ, HEADS, HEAD_DIM)
    key_rows = reduced_accuracy(low_back(matmul(seq_rows, key_weight))).reshape(SEQ, HEADS, HEAD_DIM)
    value_rows = reduced_accuracy(low_back(matmul(seq_rows, value_weight) + value_bias)).reshape(SEQ, HEADS, HEAD_DIM)
    score_scale = 1.0 / math.sqrt(HEAD_DIM)

    def attend(query_block):
        scores = low_back(jnp.einsum('qhd,khd->hqk', query_block, key_rows, precision=lax.Precision.HIGHEST)) * score_scale
        scores = jnp.where(live_slots[None, None, :], scores, -1e+30)
        row_max = lax.optimization_barrier(jnp.max(scores, axis=-1, keepdims=True))
        exponent = jnp.exp(scores - row_max)
        softmax_out = exponent / lax.optimization_barrier(jnp.sum(exponent, axis=-1, keepdims=True))
        weighted = softmax_out.reshape(HEADS, WIN, SEQ // WIN, WIN) * trainable_focus_filter[:, :, None, :]
        weighted = reduced_accuracy(weighted.reshape(HEADS, WIN, SEQ))
        return jnp.einsum('hqk,khd->qhd', weighted, value_rows, precision=lax.Precision.HIGHEST)
    contexts = lax.map(jax.checkpoint(attend), queries.reshape(SEQ // WIN, WIN, HEADS, HEAD_DIM))
    context = reduced_accuracy(low_back(contexts.reshape(SEQ, D)))
    normed = layer_norm(seq_rows + low_back(matmul(context, proj_weight)) + proj_bias, attn_gain, attn_shift)
    upper = low_back(matmul(reduced_accuracy(normed), up_weight) + up_bias)
    active = reduced_accuracy(jax.nn.gelu(upper, approximate=False))
    return layer_norm(normed + low_back(matmul(active, down_weight)) + down_bias, ffn_gain, ffn_shift)

def reference(inputs, lengths, query_weight, query_bias, key_weight, value_weight, value_bias, proj_weight, proj_bias, attn_gain, attn_shift, up_weight, up_bias, down_weight, down_bias, ffn_gain, ffn_shift, filter_couple_scores, filter_smoothing_jitter, cotangent):
    params = tuple((entry.astype(jnp.float32) for entry in (query_weight, query_bias, key_weight, value_weight, value_bias, proj_weight, proj_bias, attn_gain, attn_shift, up_weight, up_bias, down_weight, down_bias, ffn_gain, ffn_shift, filter_couple_scores)))
    draw_jitter = filter_smoothing_jitter.astype(jnp.float32)
    slot_ids = jnp.arange(SEQ, dtype=jnp.int32)

    def sequence_step(totals, pieces):
        seq_rows, upstream, length = pieces
        live_slots = slot_ids < length

        def apply(weights, row_values):
            return forward(weights, row_values, live_slots, draw_jitter)
        result, pullback = jax.vjp(apply, params, seq_rows)
        param_grads, row_grads = pullback(upstream * live_slots[:, None].astype(jnp.float32))
        totals = jax.tree.map(lambda summed, extra: summed + extra, totals, param_grads)
        return (totals, (result.astype(jnp.bfloat16), row_grads.astype(jnp.bfloat16)))
    initial = jax.tree.map(jnp.zeros_like, params)
    totals, (outputs, row_grads) = lax.scan(sequence_step, initial, (inputs.astype(jnp.float32).reshape(SEQS, SEQ, D), cotangent.astype(jnp.float32).reshape(SEQS, SEQ, D), lengths))
    return (outputs.reshape(TOKENS, D), row_grads.reshape(TOKENS, D), totals[0], totals[2], totals[3], totals[5], totals[9], totals[11], totals[1], totals[4], totals[10], totals[6], totals[12], totals[7], totals[8], totals[13], totals[14], totals[15])
```

```python
import functools
import math

import jax
import jax.numpy as jnp
from jax import lax
from jax.experimental import pallas as pl
from jax.experimental.pallas import tpu as pltpu
from jax.sharding import PartitionSpec as P

HEAD_DIM = 64
PAIR = 128


def dot(a, b, dims=(((1,), (0,)), ((), ()))):
    return lax.dot_general(a, b, dims, preferred_element_type=jnp.float32)


NT = (((1,), (1,)), ((), ()))
TN = (((0,), (0,)), ((), ()))


def head_lanes(shape, head):
    lane = lax.broadcasted_iota(jnp.int32, shape, 1)
    return (lane < HEAD_DIM) if head == 0 else (lane >= HEAD_DIM)


def masked_pair(query, key, bias, head):
    own = head_lanes(query.shape, head)
    lane = lax.broadcasted_iota(jnp.int32, query.shape, 1)
    spare = HEAD_DIM if head == 0 else 0
    one = jnp.where(lane == spare, 1.0, 0.0).astype(query.dtype)
    query_head = jnp.where(own, query, one)
    lane_k = lax.broadcasted_iota(jnp.int32, key.shape, 1)
    key_head = jnp.where(
        head_lanes(key.shape, head), key, jnp.where(lane_k == spare, bias, jnp.zeros_like(bias))
    )
    return query_head, key_head


def attend_kernel(factor, q_ref, k_ref, v_ref, bias_ref, dam_ref, ctx_ref, lse_ref):
    query, key, value, bias = q_ref[...], k_ref[...], v_ref[...], bias_ref[...]
    window = dam_ref.shape[2]
    blocks = key.shape[0] // window
    outs, logs = [], []
    for head in range(2):
        query_head, key_head = masked_pair(query, key, bias, head)
        raw = dot(query_head, key_head, NT)
        top = jnp.max(raw, axis=1, keepdims=True)
        exponent = jnp.exp2((raw - top) * factor)
        total = jnp.sum(exponent, axis=1, keepdims=True)
        low = exponent.astype(jnp.bfloat16)
        dam = dam_ref[head]
        acc = None
        for j in range(blocks):
            cols = slice(j * window, (j + 1) * window)
            part = dot(low[:, cols] * dam, value[cols])
            acc = part if acc is None else acc + part
        outs.append(acc * (1.0 / total))
        logs.append(top * factor + jnp.log2(total))
    first = head_lanes(outs[0].shape, 0)
    ctx_ref[...] = jnp.where(first, outs[0], outs[1]).astype(ctx_ref.dtype)
    lse_ref[...] = jnp.where(first, logs[0], logs[1])


def attend(joint, bias, dam, chunk, chunks):
    seq = joint.shape[0]
    width = joint.shape[1] // 3
    window = dam.shape[2]
    halves = seq // window
    pairs = width // PAIR
    tile = window // chunks
    factor = math.log2(math.e) / math.sqrt(HEAD_DIM)
    own = pl.BlockSpec((tile, PAIR), lambda p, b: (b, p))
    rows = halves * tile
    return pl.pallas_call(
        functools.partial(attend_kernel, factor),
        grid=(pairs, halves),
        in_specs=[
            pl.BlockSpec((tile, PAIR), lambda p, b: (b * chunks + chunk, p)),
            pl.BlockSpec((seq, PAIR), lambda p, b: (0, pairs + p)),
            pl.BlockSpec((seq, PAIR), lambda p, b: (0, 2 * pairs + p)),
            pl.BlockSpec((seq, PAIR), lambda p, b: (0, 0)),
            pl.BlockSpec((2, tile, window), lambda p, b: (p, chunk, 0)),
        ],
        out_specs=[own, own],
        out_shape=[
            jax.ShapeDtypeStruct((rows, width), jnp.bfloat16),
            jax.ShapeDtypeStruct((rows, width), jnp.float32),
        ],
        compiler_params=pltpu.CompilerParams(vmem_limit_bytes=40 << 20),
        cost_estimate=pl.CostEstimate(
            flops=16 * rows * seq * width,
            bytes_accessed=rows * width * 8 + seq * width * 4 + 4 * rows * window * pairs,
            transcendentals=rows * seq * width // HEAD_DIM,
        ),
        name="attend",
    )(joint, joint, joint, bias, dam)


def back_kernel(factor, scale, q_ref, k_ref, v_ref, bias_ref, dam_ref, ctx_ref, lse_ref, do_ref,
                dq_ref, dk_ref, dv_ref, gm_ref, dk_acc, dv_acc, gm_acc):
    tile_id, block_id = pl.program_id(1), pl.program_id(2)
    blocks = pl.num_programs(2)
    query, key, value, bias = q_ref[...], k_ref[...], v_ref[...], bias_ref[...]
    up = do_ref[...]
    window = dam_ref.shape[2]
    parts = key.shape[0] // window
    start = jnp.logical_and(tile_id == 0, block_id == 0)

    @pl.when(start)
    def _():
        dk_acc[...] = jnp.zeros_like(dk_acc)
        dv_acc[...] = jnp.zeros_like(dv_acc)

    @pl.when(block_id == 0)
    def _():
        gm_acc[...] = jnp.zeros_like(gm_acc)

    query_t = query.T
    up_t = up.T
    product = up.astype(jnp.float32) * ctx_ref[...].astype(jnp.float32)
    grads = []
    for head in range(2):
        own = head_lanes(query.shape, head)
        rows = slice(head * HEAD_DIM, (head + 1) * HEAD_DIM)
        query_head, key_head = masked_pair(query, key, bias, head)
        up_head = jnp.where(own, up, jnp.zeros_like(up))
        log_total = lse_ref[:, head * HEAD_DIM : head * HEAD_DIM + 1]
        delta = jnp.sum(jnp.where(own, product, 0.0), axis=1, keepdims=True)
        dam = dam_ref[head].astype(jnp.float32)
        raw = dot(query_head, key_head, NT)
        weighted_grad = dot(up_head, value, NT)
        grad_query = None
        for j in range(parts):
            cols = slice(j * window, (j + 1) * window)
            probs = jnp.exp2(raw[:, cols] * factor - log_total)
            gw = weighted_grad[:, cols]
            gm_acc[head] += probs * gw
            dv_acc[rows, cols] += dot(up_t[rows], (probs * dam).astype(jnp.bfloat16))
            ds = (probs * (gw * dam - delta)).astype(jnp.bfloat16)
            dk_acc[rows, cols] += dot(query_t[rows], ds)
            part = dot(ds, key[cols])
            grad_query = part if grad_query is None else grad_query + part
        grads.append(grad_query)
    dq_ref[...] = (jnp.where(head_lanes(query.shape, 0), grads[0], grads[1]) * scale).astype(dq_ref.dtype)

    @pl.when(block_id == blocks - 1)
    def _():
        gm_ref[...] = gm_acc[...].astype(gm_ref.dtype)

    @pl.when(jnp.logical_and(tile_id == pl.num_programs(1) - 1, block_id == blocks - 1))
    def _():
        dk_ref[...] = (dk_acc[...] * scale).T.astype(dk_ref.dtype)
        dv_ref[...] = dv_acc[...].T.astype(dv_ref.dtype)


def attend_back(joint, bias, dam, context, logs, grad_context, chunks):
    seq = joint.shape[0]
    width = joint.shape[1] // 3
    heads, _, window = dam.shape
    pairs = width // PAIR
    tile = window // chunks
    blocks = seq // window
    scale = 1.0 / math.sqrt(HEAD_DIM)
    factor = math.log2(math.e) * scale
    whole = pl.BlockSpec((seq, PAIR), lambda p, a, b: (0, p))
    natural = pl.BlockSpec((tile, PAIR), lambda p, a, b: (b * chunks + a, p))
    chunked = pl.BlockSpec((tile, PAIR), lambda p, a, b: (a * blocks + b, p))
    table = pl.BlockSpec((2, tile, window), lambda p, a, b: (p, a, 0))
    out = jax.ShapeDtypeStruct((seq, width), jnp.bfloat16)
    return pl.pallas_call(
        functools.partial(back_kernel, factor, scale),
        grid=(pairs, chunks, blocks),
        in_specs=[
            natural,
            pl.BlockSpec((seq, PAIR), lambda p, a, b: (0, pairs + p)),
            pl.BlockSpec((seq, PAIR), lambda p, a, b: (0, 2 * pairs + p)),
            pl.BlockSpec((seq, PAIR), lambda p, a, b: (0, 0)),
            table,
            chunked,
            chunked,
            chunked,
        ],
        out_specs=[natural, whole, whole, table],
        out_shape=[out, out, out, jax.ShapeDtypeStruct(dam.shape, jnp.bfloat16)],
        scratch_shapes=[
            pltpu.VMEM((PAIR, seq), jnp.float32),
            pltpu.VMEM((PAIR, seq), jnp.float32),
            pltpu.VMEM((2, tile, window), jnp.float32),
        ],
        compiler_params=pltpu.CompilerParams(vmem_limit_bytes=40 << 20),
        cost_estimate=pl.CostEstimate(
            flops=40 * seq * seq * width,
            bytes_accessed=seq * width * 20 + heads * window * window * 4,
            transcendentals=seq * seq * width // HEAD_DIM,
        ),
        name="attend_back",
    )(joint, joint, joint, bias, dam, context, logs, grad_context)


CHUNKS = 2
softening_heat = 0.5
epsilon = 1e-05


def swap(values):
    return lax.ppermute(values, "tensor", [(0, 1), (1, 0)])


def exchange(partial):
    half = partial.shape[0] // 2
    sent = jnp.concatenate([partial[half:], partial[:half]], axis=0).astype(jnp.bfloat16)
    return partial + swap(sent).astype(jnp.float32)


def layer_norm(values):
    centre = values - jnp.mean(values, axis=-1, keepdims=True)
    spread = jnp.mean(centre * centre, axis=-1, keepdims=True)
    inverse = lax.rsqrt(spread + epsilon)
    return centre * inverse, inverse


def norm_back(upstream, normal, inverse, gain):
    scaled = upstream * gain
    first_mean = jnp.mean(scaled, axis=-1, keepdims=True)
    second_mean = jnp.mean(scaled * normal, axis=-1, keepdims=True)
    return inverse * (scaled - first_mean - normal * second_mean)


def on_device(
    inputs, lengths, query_weight, query_bias, key_weight, value_weight, value_bias,
    proj_weight, proj_bias, attn_gain, attn_shift, up_weight, up_bias, down_weight,
    down_bias, ffn_gain, ffn_shift, filter_couple_scores, filter_smoothing_jitter, cotangent,
):
    half = inputs.shape[0]
    width = query_weight.shape[1]
    step = half // CHUNKS
    low = jnp.bfloat16
    full = jnp.float32
    place = lax.axis_index("tensor")
    softened = jax.nn.sigmoid((filter_couple_scores + filter_smoothing_jitter) / softening_heat)
    dam = lax.all_gather(softened.astype(low), "dp", axis=1, tiled=True)
    others = swap(inputs)
    other_cotangent = swap(cotangent)
    ids = jnp.arange(half, dtype=jnp.int32)
    slots = jnp.concatenate([ids + place * half, ids + (1 - place) * half])
    live = slots < lengths[0]
    bias = jnp.broadcast_to(jnp.where(live, 0.0, -1e30).astype(low)[:, None], (2 * half, PAIR))
    rows = jnp.concatenate([inputs, others], axis=0)
    joint_weight = jnp.concatenate([query_weight, key_weight, value_weight], axis=1)
    joint_bias = jnp.concatenate([query_bias, jnp.zeros_like(query_bias), value_bias])
    joint = (dot(rows, joint_weight) + joint_bias).astype(low)

    def pick(own, other, c):
        part = slice(c * step, (c + 1) * step)
        return jnp.concatenate([own[part], other[part]], axis=0)

    contexts, logs, sums = [], [], []
    for c in range(CHUNKS):
        context, log_total = attend(joint, bias, dam, c, CHUNKS)
        contexts.append(context)
        logs.append(log_total)
        sums.append(exchange(dot(context, proj_weight)))
    small = {}

    def count(name, values):
        small[name] = small.get(name, 0.0) + values

    root = math.sqrt(0.5)
    saved = []
    for c in range(CHUNKS):
        pre = pick(inputs, others, c).astype(full) + sums[c] + proj_bias
        normal, inverse = layer_norm(pre)
        normed = normal * attn_gain + attn_shift
        hidden = normed.astype(low)
        upper = dot(hidden, up_weight) + up_bias
        phi = 0.5 * (1.0 + lax.erf(upper * root))
        active = (upper * phi).astype(low)
        slope = (phi + upper * jnp.exp(-0.5 * upper * upper) * (1.0 / math.sqrt(2.0 * math.pi))).astype(low)
        summed = exchange(dot(active, down_weight))
        saved.append((normal, inverse, normed, hidden, active, slope, summed))
    outputs, backs = [], []
    down_grad = up_grad = None
    for c in range(CHUNKS):
        normal, inverse, normed, hidden, active, slope, summed = saved[c]
        normal_ffn, inverse_ffn = layer_norm(normed + summed + down_bias)
        outputs.append((normal_ffn[:step] * ffn_gain + ffn_shift).astype(low))
        alive = jnp.concatenate(
            [live[c * step : (c + 1) * step], live[half + c * step : half + (c + 1) * step]]
        )
        grad_out = pick(cotangent, other_cotangent, c).astype(full) * alive[:, None].astype(full)
        grad_ffn = norm_back(grad_out, normal_ffn, inverse_ffn, ffn_gain)
        count("ffn_gain", jnp.sum(grad_out[:step] * normal_ffn[:step], axis=0))
        count("ffn_shift", jnp.sum(grad_out[:step], axis=0))
        count("down_bias", jnp.sum(grad_ffn[:step], axis=0))
        grad_low = grad_ffn.astype(low)
        grad_upper = (dot(grad_low, down_weight, NT) * slope.astype(full)).astype(low)
        grad_hidden = exchange(dot(grad_upper, up_weight, NT))
        backs.append((grad_ffn, grad_hidden))
        count("up_bias", jnp.sum(grad_upper.astype(full), axis=0))
        part = dot(active, grad_low, TN)
        down_grad = part if down_grad is None else down_grad + part
        part = dot(hidden, grad_upper, TN)
        up_grad = part if up_grad is None else up_grad + part
    up_sum, down_sum = lax.psum((up_grad.astype(low), down_grad.astype(low)), "dp")
    grads_attn, grads_low = [], []
    proj_grad = None
    for c in range(CHUNKS):
        normal, inverse = saved[c][0], saved[c][1]
        grad_ffn, grad_hidden = backs[c]
        grad_normed = grad_ffn + grad_hidden
        grad_attn = norm_back(grad_normed, normal, inverse, attn_gain)
        count("attn_gain", jnp.sum(grad_normed[:step] * normal[:step], axis=0))
        count("attn_shift", jnp.sum(grad_normed[:step], axis=0))
        count("proj_bias", jnp.sum(grad_attn[:step], axis=0))
        grads_attn.append(grad_attn[:step])
        grad_low = grad_attn.astype(low)
        grads_low.append(dot(grad_low, proj_weight, NT).astype(low))
        part = dot(contexts[c], grad_low, TN)
        proj_grad = part if proj_grad is None else proj_grad + part
    grad_context = jnp.concatenate(grads_low, axis=0)
    grad_query, grad_key, grad_value, mask_grad = attend_back(
        joint, bias, dam, jnp.concatenate(contexts, axis=0), jnp.concatenate(logs, axis=0), grad_context, CHUNKS
    )
    mask_sum = lax.psum_scatter(mask_grad, "dp", scatter_dimension=1, tiled=True)
    mask_out = mask_sum.astype(full) * softened * (1.0 - softened) / softening_heat

    def back_rows(part):
        return (
            dot(grad_query[part], query_weight, NT)
            + dot(grad_key[part], key_weight, NT)
            + dot(grad_value[part], value_weight, NT)
        )

    arrived = swap(back_rows(slice(half, None)).astype(low))
    input_grad = (jnp.concatenate(grads_attn, axis=0) + back_rows(slice(0, half)) + arrived.astype(full)).astype(low)
    query_grad = dot(rows, grad_query, TN)
    key_grad = dot(rows, grad_key, TN)
    value_grad = dot(rows, grad_value, TN)
    query_bias_grad = jnp.sum(grad_query.astype(full), axis=0)
    value_bias_grad = jnp.sum(grad_value.astype(full), axis=0)
    model = inputs.shape[1]
    joined = jnp.concatenate(
        [query_bias_grad, value_bias_grad, small["up_bias"]]
        + [small[n] for n in ("proj_bias", "down_bias", "attn_gain", "attn_shift", "ffn_gain", "ffn_shift")]
    )
    table = joined.reshape(-1, model)
    extra = -table.shape[0] % 16
    table = jnp.concatenate([table, jnp.zeros((extra, model), full)], axis=0)
    proj_table = jnp.concatenate([proj_grad, table], axis=0).astype(low)
    tail = (query_grad.astype(low), key_grad.astype(low), value_grad.astype(low), proj_table)
    tail, up_sum, down_sum = lax.optimization_barrier((tail, up_sum, down_sum))
    query_sum, key_sum, value_sum, proj_table = lax.psum(tail, "dp")
    flat = proj_table[width:].astype(full).reshape(-1)
    spread = flat[2 * width + up_bias.shape[0] :][: 6 * model].reshape(6, model)
    spread = spread + swap(spread)
    return (
        jnp.concatenate(outputs, axis=0),
        input_grad,
        query_sum.astype(full),
        key_sum.astype(full),
        value_sum.astype(full),
        proj_table[:width].astype(full),
        up_sum.astype(full),
        down_sum.astype(full),
        flat[:width],
        flat[width : 2 * width],
        flat[2 * width :][: up_bias.shape[0]],
        spread[0],
        spread[1],
        spread[2],
        spread[3],
        spread[4],
        spread[5],
        mask_out,
    )


def solution(mesh):
    in_specs = (
        P(("dp", "tensor"), None),
        P("dp"),
        P(None, "tensor"),
        P("tensor"),
        P(None, "tensor"),
        P(None, "tensor"),
        P("tensor"),
        P("tensor", None),
        P(),
        P(),
        P(),
        P(None, "tensor"),
        P("tensor"),
        P("tensor", None),
        P(),
        P(),
        P(),
        P("tensor", "dp", None),
        P("tensor", "dp", None),
        P(("dp", "tensor"), None),
    )
    out_specs = (
        P(("dp", "tensor"), None),
        P(("dp", "tensor"), None),
        P(None, "tensor"),
        P(None, "tensor"),
        P(None, "tensor"),
        P("tensor", None),
        P(None, "tensor"),
        P("tensor", None),
        P("tensor"),
        P("tensor"),
        P("tensor"),
        P(),
        P(),
        P(),
        P(),
        P(),
        P(),
        P("tensor", "dp", None),
    )
    return jax.shard_map(
        on_device, mesh=mesh, in_specs=in_specs, out_specs=out_specs, check_vma=False
    )
```
